32 devices in a mesh: outer: 4 (over y, x), inner: 8 (over z, core).
Axes of the slice: x: 2, y: 2, z: 4, core: 2. Of those that a mesh axis runs over, the one named last changes fastest.
Arguments:
- ratings: bfloat16 [32768, 2048], P(('outer', 'inner')), may hold values from -4 to 4
- rating_weights: bfloat16 [32768, 2048], P(('outer', 'inner')), may hold values from 0 to 1.5, as said below
- user_counts: int32 [32768], P(('outer', 'inner')), may hold values from 16 to 96
- item_counts: int32 [8192], replicated, may hold values from 32 to 256
- users: bfloat16 [32768, 256], P(('outer', 'inner')), may hold values from -1.5 to 1.5
- user_moment: float32 [32768, 256], P(('outer', 'inner')), may hold values from -0.3 to 0.3
- items: bfloat16 [8192, 256], P(('outer', 'inner')), may hold values from -1.5 to 1.5
- item_moment: bfloat16 [8192, 256], P(('outer', 'inner')), may hold values from -0.29882812 to 0.29882812
Outputs:
- new_users: bfloat16 [32768, 256], P(('outer', 'inner'))
- new_user_moment: float32 [32768, 256], P(('outer', 'inner'))
- new_items: bfloat16 [8192, 256], P(('outer', 'inner'))
- new_item_moment: bfloat16 [8192, 256], P(('outer', 'inner'))
The draws below stay inside these ranges and needn't reach their ends.
Inputs may be any that keep to these rules, and one draw needn't show every extreme that they name: `rating_weights`: A weight is 0 exactly where the rating is not observed, else positive.
All inputs are finite; a program needn't handle non-finite values.
Results may differ from the reference program's by a relative error of at most 0.011.
Values may be sent and summed in bfloat16 or wider, within the bound.
A program may use at most 128 MiB of HBM per device.

```python
import jax
import jax.numpy as jnp
from jax import lax

NU = 1024
R = 256
IB = 256
STEPS = 8
USERS = 32768
ITEMS = 8192
N_OUTER = 4
N_INNER = 8


def draw_rating_weights(key, part):
    width = STEPS * IB
    observed = (jax.random.randint(jax.random.fold_in(key, 31), (USERS, width), 0, 8) == 0).astype(jnp.float32)
    level = jax.random.uniform(jax.random.fold_in(key, 47), (USERS, width), jnp.float32, 0.5, 1.5)
    return (observed * level).astype(jnp.bfloat16)


def touch_ends(result, own_key, smallest, top_value):
    spot = [jax.random.randint(jax.random.fold_in(own_key, axis), (), 0, length) for axis, length in enumerate(result.shape)]
    main_axis = result.shape.index(max(result.shape))
    beside = spot[:main_axis] + [(spot[main_axis] + 1) % result.shape[main_axis]] + spot[main_axis + 1:]
    return result.at[tuple(spot)].set(smallest).at[tuple(beside)].set(top_value)


def levels(own_key, dims, cuts, least, largest):
    gain = 1.0
    for axis_at, parts in cuts:
        heights = jax.random.uniform(jax.random.fold_in(jax.random.fold_in(own_key, 6), axis_at), (parts,), jnp.float32, least / len(cuts), largest / len(cuts))
        gain = gain * jnp.repeat(jnp.exp(heights), dims[axis_at] // parts).reshape((-1,) + (1,) * (len(dims) - 1 - axis_at))
    return gain


def noise(rng, shape, scale, most, cuts=(), held_as=jnp.bfloat16):
    values = scale * jax.random.normal(rng, shape, jnp.float32)
    if cuts:
        values = values * levels(rng, shape, cuts, -0.22, 0.18)
    return jnp.clip(values, -most, most).astype(held_as)


def setup_inputs(seed: int = 0) -> dict:
    seeds = jax.random.split(jax.random.key(seed), 9)
    return {
        "ratings": noise(seeds[0], (USERS, STEPS * IB), 1.0, 4.0, ((0, 32),)),
        "rating_weights": draw_rating_weights(jax.random.fold_in(seeds[8], 71), 0),
        "user_counts": touch_ends(jax.random.randint(seeds[2], (USERS,), 16, 97), jax.random.fold_in(seeds[2], 1), 16, 96).astype(jnp.int32),
        "item_counts": touch_ends(jax.random.randint(seeds[3], (ITEMS,), 32, 257), jax.random.fold_in(seeds[3], 1), 32, 256).astype(jnp.int32),
        "users": noise(seeds[4], (USERS, R), 0.25, 1.5, ((0, 32),)),
        "user_moment": noise(seeds[5], (USERS, R), 0.05, 0.3, ((0, 32),), jnp.float32),
        "items": noise(seeds[6], (ITEMS, R), 0.25, 1.5, ((0, 32),)),
        "item_moment": noise(seeds[7], (ITEMS, R), 0.05, 0.29882812, ((0, 32),)),
    }


learn_rate = 0.3
moment_rate = 0.9
decay_rate = 0.02


def misfit_of(users, items, rated, weight):
    predicted = jnp.dot(users, items.T, preferred_element_type=jnp.float32)
    return (weight * (predicted - rated.astype(jnp.float32))).astype(jnp.bfloat16)


def item_step(misfit, users, items, moment, counts):
    product = lax.dot_general(misfit, users, (((0,), (0,)), ((), ())), preferred_element_type=jnp.float32)
    grad = product / counts[:, None] + decay_rate * items.astype(jnp.float32)
    moment_new = (moment_rate * moment.astype(jnp.float32) + grad).astype(jnp.bfloat16)
    kept = lax.optimization_barrier(moment_new)
    items_new = (items.astype(jnp.float32) - learn_rate * kept.astype(jnp.float32)).astype(jnp.bfloat16)
    return items_new, moment_new


def user_step(grad_sum, users, moment, counts):
    grad = grad_sum / counts[:, None] + decay_rate * users.astype(jnp.float32)
    moment_new = moment_rate * moment + grad
    users_new = (users.astype(jnp.float32) - learn_rate * moment_new).astype(jnp.bfloat16)
    return users_new, moment_new


def reference(ratings, rating_weights, user_counts, item_counts, users, user_moment, items, item_moment):
    devices = N_OUTER * N_INNER
    rated_all = ratings.reshape(devices, NU, STEPS, IB)
    weight_all = rating_weights.reshape(devices, NU, STEPS, IB)
    ucount = user_counts.reshape(devices, NU).astype(jnp.float32)
    icount = item_counts.reshape(devices, IB).astype(jnp.float32)
    user_blocks = users.reshape(devices, NU, R)
    user_moms = user_moment.reshape(devices, NU, R)
    item_blocks = items.reshape(devices, IB, R)
    item_moms = item_moment.reshape(devices, IB, R)
    block_ids = jnp.arange(devices, dtype=jnp.int32)
    for step in range(STEPS):
        def one_device(packed):
            ublock, umom, iblock, imom, rated, weight, ucnt, icnt = packed
            misfit = misfit_of(ublock, iblock, rated, weight.astype(jnp.float32))
            new_items, new_imom = item_step(misfit, ublock, iblock, imom, icnt)
            grad_sum = jnp.dot(misfit, iblock, preferred_element_type=jnp.float32)
            new_users, new_umom = user_step(grad_sum, ublock, umom, ucnt)
            return new_users, new_umom, new_items, new_imom

        user_blocks, user_moms, item_blocks, item_moms = lax.map(one_device, (user_blocks, user_moms, item_blocks, item_moms, rated_all[:, :, step], weight_all[:, :, step], ucount, icount[block_ids]))
        if step < STEPS - 1:
            axis_used = 0 if step == STEPS // 2 - 1 else 1
            item_blocks = jnp.roll(item_blocks.reshape(N_OUTER, N_INNER, IB, R), 1, axis=axis_used).reshape(devices, IB, R)
            item_moms = jnp.roll(item_moms.reshape(N_OUTER, N_INNER, IB, R), 1, axis=axis_used).reshape(devices, IB, R)
            block_ids = jnp.roll(block_ids.reshape(N_OUTER, N_INNER), 1, axis=axis_used).reshape(devices)
    return (user_blocks.reshape(USERS, R), user_moms.reshape(USERS, R), item_blocks.reshape(ITEMS, R), item_moms.reshape(ITEMS, R))
```

```python
import functools

import jax
import jax.numpy as jnp
from jax import lax
from jax.experimental import pallas as pl
from jax.experimental.pallas import tpu as pltpu
from jax.sharding import PartitionSpec as P

STEPS = 8
CHUNKS = 2
TILE = 256
LANES = 128
MESH = pl.DeviceIdType.MESH

learn_rate = 0.3
moment_rate = 0.9
decay_rate = 0.02


def kernel(
    n_outer, n_inner,
    x_hbm, w_hbm, uc_hbm, ic_hbm, u_hbm, p_hbm, v_hbm, q_hbm,
    u_out, p_out, v_out, q_out,
    x, w, uc, ic, u, ut, p, v0, q0, vt, qt, vn, qn, mis, rcu, counts,
    x_sem, w_sem, in_sem, send_sem, recv_sem, out_sem,
):
    outer = lax.axis_index("outer")
    inner = lax.axis_index("inner")
    i_right, i_left = lax.rem(inner + 1, n_inner), lax.rem(inner + n_inner - 1, n_inner)
    o_right, o_left = lax.rem(outer + 1, n_outer), lax.rem(outer + n_outer - 1, n_outer)

    users, rank = u.shape
    block = v0.shape[0]
    part = block // CHUNKS
    tile = min(TILE, users)

    def load(src, dst, sem):
        copy = pltpu.make_async_copy(src, dst, sem)
        copy.start()
        return copy

    v_load = load(v_hbm, v0, in_sem.at[0])
    u_load = load(u_hbm, u, in_sem.at[1])
    loads = []
    for s in range(STEPS):
        cols = slice(s * block, (s + 1) * block)
        loads.append((
            load(x_hbm.at[:, cols], x.at[s], x_sem.at[s]),
            load(w_hbm.at[:, cols], w.at[s], w_sem.at[s]),
        ))
        if s == 0:
            q_load = load(q_hbm, q0, in_sem.at[2])
            ic_load = load(ic_hbm, ic, in_sem.at[3])
            uc_load = load(uc_hbm, uc, in_sem.at[4])
            p_load = load(p_hbm, p, in_sem.at[5])

    barrier = pltpu.get_barrier_semaphore()
    for where in ((outer, i_left), (outer, i_right), (o_left, inner), (o_right, inner)):
        pl.semaphore_signal(barrier, inc=1, device_id=where, device_id_type=MESH)

    v_load.wait()
    vt[0] = v0[...].T
    u_load.wait()
    for t in range(users // tile):
        rows = slice(t * tile, (t + 1) * tile)
        ut[:, rows] = u[rows, :].T
    q_load.wait()
    qt[0] = q0[...].T

    ic_load.wait()
    per = block // LANES
    for s in range(STEPS):
        late = 1 if s >= STEPS // 2 else 0
        o_from = lax.rem(outer - late + n_outer, n_outer)
        i_from = lax.rem(inner - (s - late) + n_inner * STEPS, n_inner)
        first = (o_from * n_inner + i_from) * per
        for j in range(per):
            row = ic[pl.ds(first + j, 1), :].astype(jnp.float32)
            counts[s : s + 1, j * LANES : (j + 1) * LANES] = 1.0 / row
    uc_load.wait()
    flipped = (1.0 / uc[...].astype(jnp.float32)).T
    for j in range(users // LANES):
        rcu[j * LANES : (j + 1) * LANES, :] = jnp.broadcast_to(flipped[:, j : j + 1], (LANES, LANES))

    sends = []
    outs = []
    arrivals = [None]
    for s in range(STEPS):
        last = s == STEPS - 1
        if s == STEPS // 2 - 1:
            target = (o_right, inner)
        else:
            target = (outer, i_right)
        if s == 0:
            loads[0][0].wait()
            loads[0][1].wait()
        else:
            loads[s][0].wait()
            loads[s][1].wait()
        copies = []
        for k in range(CHUNKS):
            cols = slice(k * part, (k + 1) * part)
            if s > 0:
                arrivals[s][k][0].wait_recv()
            items = vt[s, :, cols]
            for t in range(users // tile):
                rows = slice(t * tile, (t + 1) * tile)
                pred = jnp.dot(u[rows, :], items, preferred_element_type=jnp.float32)
                rated = x[s, rows, cols].astype(jnp.float32)
                weight = w[s, rows, cols].astype(jnp.float32)
                mis[rows, cols] = (weight * (pred - rated)).astype(jnp.bfloat16)
            product = jnp.dot(ut[...], mis[:, cols], preferred_element_type=jnp.float32)
            if s > 0:
                arrivals[s][k][1].wait_recv()
            old = items.astype(jnp.float32)
            grad = product * counts[s : s + 1, cols] + decay_rate * old
            moment = (moment_rate * qt[s, :, cols].astype(jnp.float32) + grad).astype(jnp.bfloat16)
            qn[s, :, cols] = moment
            vn[s, :, cols] = (old - learn_rate * moment.astype(jnp.float32)).astype(jnp.bfloat16)
            if not last:
                if s == 0 and k == 0:
                    pl.semaphore_wait(barrier, 4)
                pair = []
                for j, (src, dst) in enumerate(((vn, vt), (qn, qt))):
                    copy = pltpu.make_async_remote_copy(
                        src_ref=src.at[s, :, cols],
                        dst_ref=dst.at[s + 1, :, cols],
                        send_sem=send_sem.at[s, k, j],
                        recv_sem=recv_sem.at[s, k, j],
                        device_id=target,
                        device_id_type=MESH,
                    )
                    copy.start()
                    pair.append(copy)
                copies.append(pair)
            else:
                v0[cols, :] = vn[s, :, cols].T
                q0[cols, :] = qn[s, :, cols].T
                for j, (src, dst) in enumerate(((v0, v_out), (q0, q_out))):
                    outs.append(load(src.at[cols], dst.at[cols], out_sem.at[0, 2 * k + j]))
        arrivals.append(copies)
        sends.append(copies)
        if s == 0:
            p_load.wait()
        for t in range(users // tile):
            rows = slice(t * tile, (t + 1) * tile)
            total = lax.dot_general(
                mis[rows, :], vt[s], (((1,), (1,)), ((), ())), preferred_element_type=jnp.float32
            )
            old = u[rows, :].astype(jnp.float32)
            scale = jnp.concatenate([rcu[rows, :]] * (rank // LANES), axis=1)
            moment = moment_rate * p[rows, :] + (total * scale + decay_rate * old)
            p[rows, :] = moment
            new = (old - learn_rate * moment).astype(jnp.bfloat16)
            u[rows, :] = new
            if last:
                outs.append(load(u.at[rows], u_out.at[rows], out_sem.at[1, t]))
                outs.append(load(p.at[rows], p_out.at[rows], out_sem.at[2, t]))
            else:
                ut[:, rows] = new.T
    for copies in sends:
        for pair in copies:
            for copy in pair:
                copy.wait_send()
    for copy in outs:
        copy.wait()


def body(ratings, rating_weights, user_counts, item_counts, users, user_moment, items, item_moment):
    n_outer = lax.axis_size("outer")
    n_inner = lax.axis_size("inner")
    n_users, rank = users.shape
    block = items.shape[0]
    n_items = item_counts.shape[0]
    tiles = max(n_users // min(TILE, n_users), 2 * CHUNKS)
    bf16, f32, i32 = jnp.bfloat16, jnp.float32, jnp.int32
    return pl.pallas_call(
        functools.partial(kernel, n_outer, n_inner),
        out_shape=(
            jax.ShapeDtypeStruct(users.shape, bf16),
            jax.ShapeDtypeStruct(user_moment.shape, f32),
            jax.ShapeDtypeStruct(items.shape, bf16),
            jax.ShapeDtypeStruct(item_moment.shape, bf16),
        ),
        in_specs=[pl.BlockSpec(memory_space=pltpu.HBM)] * 8,
        out_specs=(pl.BlockSpec(memory_space=pl.ANY),) * 4,
        scratch_shapes=[
            pltpu.VMEM((STEPS, n_users, block), bf16),
            pltpu.VMEM((STEPS, n_users, block), bf16),
            pltpu.VMEM((n_users // LANES, LANES), i32),
            pltpu.VMEM((n_items // LANES, LANES), i32),
            pltpu.VMEM((n_users, rank), bf16),
            pltpu.VMEM((rank, n_users), bf16),
            pltpu.VMEM((n_users, rank), f32),
            pltpu.VMEM((block, rank), bf16),
            pltpu.VMEM((block, rank), bf16),
            pltpu.VMEM((STEPS, rank, block), bf16),
            pltpu.VMEM((STEPS, rank, block), bf16),
            pltpu.VMEM((STEPS, rank, block), bf16),
            pltpu.VMEM((STEPS, rank, block), bf16),
            pltpu.VMEM((n_users, block), bf16),
            pltpu.VMEM((n_users, LANES), f32),
            pltpu.VMEM((STEPS, block), f32),
            pltpu.SemaphoreType.DMA((STEPS,)),
            pltpu.SemaphoreType.DMA((STEPS,)),
            pltpu.SemaphoreType.DMA((6,)),
            pltpu.SemaphoreType.DMA((STEPS, CHUNKS, 2)),
            pltpu.SemaphoreType.DMA((STEPS, CHUNKS, 2)),
            pltpu.SemaphoreType.DMA((3, tiles)),
        ],
        compiler_params=pltpu.CompilerParams(
            collective_id=0, has_side_effects=True, vmem_limit_bytes=48 * 1024 * 1024
        ),
    )(
        ratings,
        rating_weights,
        user_counts.reshape(n_users // LANES, LANES),
        item_counts.reshape(n_items // LANES, LANES),
        users,
        user_moment,
        items,
        item_moment,
    )


def solution(mesh):
    spread = P(("outer", "inner"), None)
    in_specs = (spread, spread, P(("outer", "inner")), P(), spread, spread, spread, spread)
    return jax.shard_map(
        body, mesh=mesh, in_specs=in_specs, out_specs=(spread,) * 4, check_vma=False
    )
```
